32 devices in a mesh: freq: 8 (over y, x, core), feed: 4 (over z).
Axes of the slice: x: 2, y: 2, z: 4, core: 2. Of those that a mesh axis runs over, the one named last changes fastest.
Arguments:
- voltages: int32 [32, 2048, 2, 768], P(None, ('feed', 'freq')), may hold values from -127 to 127
- gains: float32 [2, 32, 2048], P(None, None, ('feed', 'freq')), may hold values from -0.06 to 0.06
Outputs:
- visibilities: float32 [32, 2, 2048, 2048], P('freq', None, 'feed')
The draws below stay inside these ranges and needn't reach their ends.
All inputs are finite; a program needn't handle non-finite values.
Results may differ from the reference program's by a relative error of at most 0.0031.
Values may be sent and summed in bfloat16 or wider, within the bound.
A program may use at most 192 MiB of HBM per device.

```python
import jax
import jax.numpy as jnp
from jax import lax

FEEDS = 2048
TIME = 768
CHAN = 32


def set_ends(array, rng, low, top_value):
    place = [jax.random.randint(jax.random.fold_in(rng, axis), (), 0, length) for axis, length in enumerate(array.shape)]
    longest = array.shape.index(max(array.shape))
    beside = place[:longest] + [(place[longest] + 1) % array.shape[longest]] + place[longest + 1:]
    return array.at[tuple(place)].set(low).at[tuple(beside)].set(top_value)


def block_scale(rng, dims, shards, least, top_value):
    loudness = 1.0
    for position, blocks in shards:
        draws = jax.random.uniform(jax.random.fold_in(jax.random.fold_in(rng, 6), position), (blocks,), jnp.float32, least / len(shards), top_value / len(shards))
        loudness = loudness * jnp.repeat(jnp.exp(draws), dims[position] // blocks).reshape((-1,) + (1,) * (len(dims) - 1 - position))
    return loudness


def gaussian(rng, dims, scale, limit, cuts=(), held_as=jnp.bfloat16):
    values = scale * jax.random.normal(rng, dims, jnp.float32)
    if cuts:
        values = values * block_scale(rng, dims, cuts, -0.22, 0.18)
    return jnp.clip(values, -limit, limit).astype(held_as)


def setup_inputs(seed: int = 0) -> dict:
    key_list = jax.random.split(jax.random.key(seed), 3)
    voltages = set_ends(jax.random.randint(key_list[0], (CHAN, FEEDS, 2, TIME), -127, 128), jax.random.fold_in(key_list[0], 1), -127, 127).astype(jnp.int32)
    gains = gaussian(key_list[1], (2, CHAN, FEEDS), 0.01, 0.06, ((2, 32),), jnp.float32)
    return {"voltages": voltages, "gains": gains}


def reference(voltages, gains):
    volt_real = voltages[:, :, 0, :].astype(jnp.float32)
    volt_imag = voltages[:, :, 1, :].astype(jnp.float32)
    gain_real = gains[0][:, :, None]
    gain_imag = gains[1][:, :, None]
    eq_real = gain_real * volt_real - gain_imag * volt_imag
    eq_imag = gain_real * volt_imag + gain_imag * volt_real
    equalized = jnp.stack([eq_real, eq_imag], axis=2).astype(jnp.bfloat16)

    def per_channel(block):
        columns = block.reshape(FEEDS, 2 * TIME)
        swapped = jnp.concatenate([block[:, 1, :], -block[:, 0, :]], axis=1)
        left_side = jnp.concatenate([columns, swapped], axis=0)
        result = jnp.dot(left_side, columns.T, preferred_element_type=jnp.float32)
        return result.reshape(2, FEEDS, FEEDS) * (1.0 / TIME)

    return lax.map(per_channel, equalized)
```

```python
import jax
import jax.numpy as jnp
from jax import lax
from jax.sharding import PartitionSpec as P

def stack_rows(own_rows, samples):
    real_part = own_rows[..., :samples]
    imag_part = own_rows[..., samples:]
    swapped = jnp.concatenate([imag_part, -real_part], axis=-1)
    return jnp.stack([own_rows, swapped], axis=0)


def correlate(stacked, columns, samples):
    product = jnp.einsum("qrk,fk->qrf", stacked, columns, preferred_element_type=jnp.float32)
    return product * (1.0 / samples)


def ring_blocks(own, count):
    forward = [(source, (source + 1) % count) for source in range(count)]
    backward = [(source, (source - 1) % count) for source in range(count)]
    half = own.shape[0] // 2
    pieces = [(0, 0, own)]
    from_left = from_right = own
    for step in range(1, count):
        if 2 * step > count:
            break
        if 2 * step == count:
            pieces.append((-step, 0, lax.ppermute(from_left[:half], "feed", forward)))
            pieces.append((-step, half, lax.ppermute(from_right[half:], "feed", backward)))
        else:
            from_left = lax.ppermute(from_left, "feed", forward)
            from_right = lax.ppermute(from_right, "feed", backward)
            pieces.append((-step, 0, from_left))
            pieces.append((step, 0, from_right))
    return pieces


def per_device(voltages, gains):
    channels, local_feeds, _, samples = voltages.shape
    freq_count = lax.axis_size("freq")
    feed_count = lax.axis_size("feed")
    position = lax.axis_index("feed")
    owned = channels // freq_count
    rows = local_feeds * freq_count
    volts = voltages.reshape(freq_count, owned, local_feeds, 2, samples)
    scale = gains.reshape(2, freq_count, owned, local_feeds)[..., None]
    visibilities = jnp.zeros((owned, 2, rows, rows * feed_count), jnp.float32)
    for channel in range(owned):
        volt_real = volts[:, channel, :, 0].astype(jnp.float32)
        volt_imag = volts[:, channel, :, 1].astype(jnp.float32)
        gain_real = scale[0, :, channel]
        gain_imag = scale[1, :, channel]
        eq_real = gain_real * volt_real - gain_imag * volt_imag
        eq_imag = gain_real * volt_imag + gain_imag * volt_real
        blocks = jnp.concatenate([eq_real, eq_imag], axis=-1).astype(jnp.bfloat16)
        arrived = lax.all_to_all(blocks, "freq", split_axis=0, concat_axis=0, tiled=True)
        own_rows = arrived.reshape(rows, 2 * samples)
        stacked = stack_rows(own_rows, samples)
        for offset, start, block in ring_blocks(own_rows, feed_count):
            owner = lax.rem(position + offset + feed_count, feed_count)
            visibilities = lax.dynamic_update_slice(
                visibilities,
                correlate(stacked, block, samples)[None],
                (channel, 0, 0, owner * rows + start),
            )
    return visibilities


def solution(mesh):
    in_specs = (P(None, ("feed", "freq"), None, None), P(None, None, ("feed", "freq")))
    out_specs = P("freq", None, "feed", None)
    return jax.shard_map(
        per_device, mesh=mesh, in_specs=in_specs, out_specs=out_specs, check_vma=False
    )
```
